32 devices in a mesh: shots: 2 (over y), rx: 4 (over z), ta: 2 (over x), af: 2 (over core).
Axes of the slice: x: 2, y: 2, z: 4, core: 2. Of those that a mesh axis runs over, the one named last changes fastest.
Arguments:
- traces: bfloat16 [4096, 512], P(('shots', 'rx'), ('ta', 'af')), parts along dimension 0, may hold values from -6 to 6
- slopes: int32 [512], replicated, may hold values from 0 to 1023
- offsets: int32 [4096], P('shots'), parts along dimension 0, may hold values from 1 to 4095
- live: int32 [4096], P('shots'), parts along dimension 0, may hold values 0 or 1
Outputs:
- stack: float32 [1024, 512], P(('shots', 'rx'), ('ta', 'af')), parts along dimension 0
- coherence: float32 [1024, 512], P(('shots', 'rx'), ('ta', 'af')), parts along dimension 0
- peak_values: float32 [1024], P(('shots', 'rx')), parts along dimension 0
The draws below stay inside these ranges and needn't reach their ends.
There are 2 independent parts, one for each index of `shots`. The reference program is written for one: setup_inputs(seed, part) draws one part's arguments, and reference() takes and returns one part's arrays. A program takes and returns all parts, laid end to end along the dimension named above; an argument that names none is the same for every part. Nothing has to cross between parts.
Inputs may be any that keep to these rules, and one draw needn't show every extreme that they name: delays are below 64: (slopes * offsets) // 65536 < 64.
All inputs are finite; a program needn't handle non-finite values.
Results may differ from the reference program's by a relative error of at most 0.0003.
Values may be sent and summed in bfloat16 or wider, within the bound.
A program may use at most 64 MiB of HBM per device.

```python
import jax
import jax.numpy as jnp
from jax import lax

RECV = 2048
SLOWS = 512
SPAN = 64
WIN = 16
NT = 512


def with_ends(values, rng, smallest, largest):
    index_at = [jax.random.randint(jax.random.fold_in(rng, axis), (), 0, length) for axis, length in enumerate(values.shape)]
    widest = values.shape.index(max(values.shape))
    neighbour = index_at[:widest] + [(index_at[widest] + 1) % values.shape[widest]] + index_at[widest + 1:]
    return values.at[tuple(index_at)].set(smallest).at[tuple(neighbour)].set(largest)


def steps_of(key, extent, cuts, smallest, high):
    factor_of = 1.0
    for position, shards_of in cuts:
        heights = jax.random.uniform(jax.random.fold_in(jax.random.fold_in(key, 6), position), (shards_of,), jnp.float32, smallest / len(cuts), high / len(cuts))
        factor_of = factor_of * jnp.repeat(jnp.exp(heights), extent[position] // shards_of).reshape((-1,) + (1,) * (len(extent) - 1 - position))
    return factor_of


def gaussian(key, extent, scale, limit, shards=(), held_as=jnp.bfloat16):
    result = scale * jax.random.normal(key, extent, jnp.float32)
    if shards:
        result = result * steps_of(key, extent, shards, -0.22, 0.18)
    return jnp.clip(result, -limit, limit).astype(held_as)


def setup_inputs(seed: int = 0, part: int = 0) -> dict:
    key_of = jax.random.split(jax.random.key(seed), 5)
    part_splits = jax.random.split(jax.random.fold_in(key_of[4], part), 5)
    traces = gaussian(part_splits[0], (RECV, NT), 1.0, 6.0, ((0, 4), (1, 4)))
    slopes = with_ends(jax.random.randint(key_of[1], (SLOWS,), 0, 16 * SPAN), jax.random.fold_in(key_of[1], 1), 0, (16 * SPAN) - 1).astype(jnp.int32)
    offsets = with_ends(jax.random.randint(part_splits[2], (RECV,), 1, 4096), jax.random.fold_in(part_splits[2], 1), 1, 4095).astype(jnp.int32)
    live = with_ends((jax.random.randint(part_splits[3], (RECV,), 0, 8) < 7).astype(jnp.int32), jax.random.fold_in(part_splits[3], 1), 0, 1)
    return dict(traces=traces, slopes=slopes, offsets=offsets, live=live)


def reference(traces, slopes, offsets, live):
    delays = (slopes[:, None] * offsets[None, :]) // 65536
    weighted = traces * live.astype(jnp.bfloat16)[:, None]
    squares = (weighted.astype(jnp.float32) ** 2).astype(jnp.bfloat16)
    padded_x = jnp.pad(weighted, ((0, 0), (0, SPAN)))
    padded_s = jnp.pad(squares, ((0, 0), (0, SPAN)))

    def lag_step(lag_index, carry):
        stack_acc, energy_acc = carry
        onehot = (delays == lag_index).astype(jnp.bfloat16)
        part_x = lax.dynamic_slice_in_dim(padded_x, lag_index, NT, 1)
        part_s = lax.dynamic_slice_in_dim(padded_s, lag_index, NT, 1)
        stack_acc = stack_acc + jnp.dot(onehot, part_x, preferred_element_type=jnp.float32)
        energy_acc = energy_acc + jnp.dot(onehot, part_s, preferred_element_type=jnp.float32)
        return stack_acc, energy_acc

    zeros = jnp.zeros((SLOWS, NT), jnp.float32)
    stack, energy = lax.fori_loop(0, SPAN, lag_step, (zeros, zeros))
    long_stack = jnp.pad(stack, ((0, 0), (0, WIN)))
    long_energy = jnp.pad(energy, ((0, 0), (0, WIN)))
    power_sum = jnp.zeros((SLOWS, NT), jnp.float32)
    energy_sum = jnp.zeros((SLOWS, NT), jnp.float32)
    for lag_index in range(WIN):
        power_sum = power_sum + long_stack[:, lag_index:lag_index + NT] ** 2
        energy_sum = energy_sum + long_energy[:, lag_index:lag_index + NT]
    coherence = power_sum / jnp.maximum(energy_sum, 1.0)
    peak_values = jnp.max(coherence, axis=1)
    return stack, coherence, peak_values
```

```python
import functools

import jax
import jax.numpy as jnp
from jax import lax
from jax.experimental import pallas as pl
from jax.experimental.pallas import tpu as pltpu
from jax.sharding import PartitionSpec as P

SPAN = 64
WIN = 16
STEP = 8
EDGE = SPAN + WIN
MESH = pl.DeviceIdType.MESH
F32 = jnp.float32
BF16 = jnp.bfloat16


def window_sum(rows, width):
    reach = 1
    while reach < width:
        rows = rows[:-reach] + rows[reach:]
        reach *= 2
    return rows


def kernel(
    n_rx, n_ta, n_af, subs, pair,
    traces_hbm, slopes_hbm, offsets_hbm, live_hbm,
    stack_ref, coherence_ref, peak_ref,
    slopes_ref, offsets_ref, live_ref,
    held, delays, long, left, total, edge_in, top, top_in,
    in_sem, small_sem, gather_recv, right_send, left_send,
    edge_send, edge_recv, top_send, top_recv,
):
    blocks = n_ta * n_af
    sub_rows, block_len = held.shape[2:]
    own_slows = delays.shape[2]
    tall = block_len + STEP
    rx = lax.axis_index("rx")
    block = lax.axis_index("ta") * n_af + lax.axis_index("af")
    has_previous = block > 0
    has_next = block < blocks - 1
    has_left = rx > 0
    has_right = rx < n_rx - 1

    def at_block(number):
        return {"ta": lax.div(number, n_af), "af": lax.rem(number, n_af)}

    previous = at_block(jnp.maximum(block - 1, 0))
    block_peers = [at_block(lax.rem(block + step, blocks)) for step in range(1, blocks)]

    barrier = pltpu.get_barrier_semaphore()

    @pl.when(has_left)
    def _():
        pl.semaphore_signal(barrier, inc=1, device_id={"rx": rx - 1}, device_id_type=MESH)

    @pl.when(has_right)
    def _():
        pl.semaphore_signal(barrier, inc=1, device_id={"rx": rx + 1}, device_id_type=MESH)

    for peer in block_peers:
        pl.semaphore_signal(barrier, inc=1, device_id=peer, device_id_type=MESH)

    small = [
        pltpu.make_async_copy(source, target, small_sem.at[index])
        for index, (source, target) in enumerate(
            [(slopes_hbm, slopes_ref), (offsets_hbm, offsets_ref), (live_hbm, live_ref)])
    ]
    own = [
        pltpu.make_async_copy(
            traces_hbm.at[pl.ds(sub * sub_rows, sub_rows)], held.at[rx, sub], in_sem.at[sub])
        for sub in range(subs)
    ]
    for copy in small + own:
        copy.start()

    def to_right(source, sub):
        return pltpu.make_async_remote_copy(
            src_ref=held.at[source, sub], dst_ref=held.at[source, sub],
            send_sem=right_send.at[source, sub], recv_sem=gather_recv.at[source, sub],
            device_id={"rx": jnp.minimum(rx + 1, n_rx - 1)}, device_id_type=MESH,
        )

    def to_left(source, sub):
        return pltpu.make_async_remote_copy(
            src_ref=held.at[source, sub], dst_ref=held.at[source, sub],
            send_sem=left_send.at[source, sub], recv_sem=gather_recv.at[source, sub],
            device_id={"rx": jnp.maximum(rx - 1, 0)}, device_id_type=MESH,
        )

    total[...] = jnp.zeros_like(total)
    long[0:STEP] = jnp.zeros((STEP, sub_rows), F32)
    long[block_len + STEP:] = jnp.zeros((STEP, sub_rows), F32)

    @pl.when(jnp.logical_not(has_next))
    def _():
        edge_in[...] = jnp.zeros_like(edge_in)

    for copy in small:
        copy.wait()

    near = jnp.where(has_left, 1, 0) + jnp.where(has_right, 1, 0)
    pl.semaphore_wait(barrier, near + blocks - 1)
    for sub in range(subs):
        own[sub].wait()

        @pl.when(has_right)
        def _():
            to_right(rx, sub).start()

        @pl.when(has_left)
        def _():
            to_left(rx, sub).start()

    slopes = slopes_ref[pl.ds(rx, 1), :].astype(F32)

    def set_delays(index, carry):
        lanes = pl.ds(pl.multiple_of(index * sub_rows, sub_rows), sub_rows)
        offsets = offsets_ref[:, lanes].astype(F32)
        marked = jnp.where(live_ref[:, lanes] != 0, offsets, 65536.0)
        column = jnp.broadcast_to(marked, (128, sub_rows)).T
        column = jnp.concatenate([column] * (-(-own_slows // 128)), axis=1)[:, :own_slows]
        delay = jnp.floor(column * slopes * (1.0 / 65536.0))
        delays[index] = jnp.where(column < 65536.0, delay, 127.0).astype(BF16)
        return carry

    lax.fori_loop(0, n_rx * subs, set_delays, 0)

    both = jnp.minimum(rx, n_rx - 1 - rx)

    def item_at(number):
        ahead = number - subs
        late = ahead - 2 * subs * both
        paired = late < 0
        spot = jnp.maximum(ahead, 0)
        tail = jnp.maximum(late, 0)
        distance = jnp.where(paired, lax.div(spot, 2 * subs), both + lax.div(tail, subs)) + 1
        sub = jnp.where(paired, lax.div(lax.rem(spot, 2 * subs), 2), lax.rem(tail, subs))
        leftward = jnp.where(paired, 1 - lax.rem(spot, 2), jnp.where(rx > n_rx - 1 - rx, 1, 0))
        distance = jnp.where(leftward == 1, -distance, distance)
        mine = number < subs
        return jnp.where(mine, rx, rx + distance), jnp.where(mine, number, sub)

    def exchange(step):
        distance = lax.div(step, subs) + 1
        sub = lax.rem(step, subs)
        before = jnp.maximum(rx - distance, 0)
        after = jnp.minimum(rx + distance, n_rx - 1)

        @pl.when(rx - distance >= 0)
        def _():
            to_right(before, sub).wait_recv()

            @pl.when(has_right)
            def _():
                to_right(before, sub).start()

        @pl.when(rx + distance < n_rx)
        def _():
            to_left(after, sub).wait_recv()

            @pl.when(has_left)
            def _():
                to_left(after, sub).start()

    def add_item(number, carry):
        @pl.when(number >= subs)
        def _():
            exchange(number - subs)

        source, sub = item_at(number)
        long[STEP:STEP + block_len] = held[source, sub].astype(F32).T
        delay = delays[source * subs + sub]
        for lag in range(STEP):
            samples = long[lag:lag + tall]
            left[:, lag * sub_rows:(lag + 1) * sub_rows] = jnp.concatenate(
                [samples, samples * samples], axis=0).astype(BF16)
        for first in range(0, SPAN // STEP, pair):
            right = [
                jnp.concatenate([
                    jnp.where(delay == jnp.asarray(STEP * (first + turn) + lag, BF16),
                              jnp.asarray(1, BF16), jnp.asarray(0, BF16))
                    for turn in range(pair)], axis=1)
                for lag in range(STEP)
            ]
            product = jnp.dot(left[...], jnp.concatenate(right, axis=0),
                              preferred_element_type=F32)
            for turn in range(pair):
                top_row = SPAN - STEP * (first + turn + 1)
                lanes = slice(turn * own_slows, (turn + 1) * own_slows)
                total[0, top_row:top_row + tall] += product[:tall, lanes]
                total[1, top_row:top_row + tall] += product[tall:, lanes]
        return carry

    lax.fori_loop(0, n_rx * subs, add_item, 0)

    pass_edge = pltpu.make_async_remote_copy(
        src_ref=total.at[:, pl.ds(0, EDGE)], dst_ref=edge_in,
        send_sem=edge_send, recv_sem=edge_recv,
        device_id=previous, device_id_type=MESH,
    )

    @pl.when(has_previous)
    def _():
        pass_edge.start()

    @pl.when(has_next)
    def _():
        pass_edge.wait_recv()

    near_rows = block_len - SPAN

    def whole(kind):
        return jnp.concatenate([
            total[kind, SPAN:SPAN + near_rows],
            total[kind, SPAN + near_rows:] + edge_in[kind, 0:SPAN],
            edge_in[kind, SPAN:],
        ], axis=0)

    stack, energy = whole(0), whole(1)
    power_sum = window_sum(stack * stack, WIN)[:block_len]
    energy_sum = window_sum(energy, WIN)[:block_len]
    coherence = power_sum / jnp.maximum(energy_sum, 1.0)
    peak = jnp.max(coherence, axis=0, keepdims=True)
    top[...] = peak
    tops = []
    for step, peer in enumerate(block_peers):
        tops.append(pltpu.make_async_remote_copy(
            src_ref=top, dst_ref=top_in.at[step],
            send_sem=top_send.at[step], recv_sem=top_recv.at[step],
            device_id=peer, device_id_type=MESH,
        ))
        tops[-1].start()
    stack_ref[...] = stack[:block_len].T
    coherence_ref[...] = coherence.T

    for source in range(n_rx):
        for sub in range(subs):
            @pl.when(jnp.logical_and(has_right, source <= rx))
            def _():
                to_right(source, sub).wait_send()

            @pl.when(jnp.logical_and(has_left, source >= rx))
            def _():
                to_left(source, sub).wait_send()

    @pl.when(has_previous)
    def _():
        pass_edge.wait_send()

    for step, copy in enumerate(tops):
        copy.wait_recv()
        peak = jnp.maximum(peak, top_in[step])
    peak_ref[...] = peak
    for copy in tops:
        copy.wait_send()


def emit(stack_ref, coherence_ref, peak_ref, stack_hbm, coherence_hbm, peak_hbm, sem):
    copies = [
        pltpu.make_async_copy(source, target, sem.at[index])
        for index, (source, target) in enumerate(
            [(stack_ref, stack_hbm), (coherence_ref, coherence_hbm), (peak_ref, peak_hbm)])
    ]
    for copy in copies:
        copy.start()
    for copy in copies:
        copy.wait()


def solution(mesh):
    n_rx, n_ta, n_af = (mesh.shape[name] for name in ("rx", "ta", "af"))

    def on_device(traces, slopes, offsets, live):
        local_rows, block_len = traces.shape
        subs = 2 if local_rows % 512 == 0 else 1
        sub_rows = local_rows // subs
        own_slows = slopes.shape[0] // n_rx
        pair = min(max(256 // own_slows, 1), SPAN // STEP)
        items = n_rx * subs
        blocks = n_ta * n_af
        tall = block_len + STEP
        dma = pltpu.SemaphoreType.DMA
        vmem = pl.BlockSpec(memory_space=pltpu.VMEM)
        anywhere = pl.BlockSpec(memory_space=pl.ANY)
        shapes = (
            jax.ShapeDtypeStruct((own_slows, block_len), F32),
            jax.ShapeDtypeStruct((own_slows, block_len), F32),
            jax.ShapeDtypeStruct((1, own_slows), F32),
        )
        results = pl.pallas_call(
            functools.partial(kernel, n_rx, n_ta, n_af, subs, pair),
            out_shape=shapes,
            in_specs=[anywhere] * 4,
            out_specs=(vmem,) * 3,
            scratch_shapes=[
                pltpu.VMEM((n_rx, own_slows), jnp.int32),
                pltpu.VMEM((1, n_rx * local_rows), jnp.int32),
                pltpu.VMEM((1, n_rx * local_rows), jnp.int32),
                pltpu.VMEM((n_rx, subs, sub_rows, block_len), BF16),
                pltpu.VMEM((items, sub_rows, own_slows), BF16),
                pltpu.VMEM((block_len + 2 * STEP, sub_rows), F32),
                pltpu.VMEM((2 * tall, STEP * sub_rows), BF16),
                pltpu.VMEM((2, block_len + SPAN, own_slows), F32),
                pltpu.VMEM((2, EDGE, own_slows), F32),
                pltpu.VMEM((1, own_slows), F32),
                pltpu.VMEM((max(blocks - 1, 1), 1, own_slows), F32),
                dma((subs,)), dma((3,)), dma((n_rx, subs)), dma((n_rx, subs)), dma((n_rx, subs)),
                dma, dma,
                dma((max(blocks - 1, 1),)), dma((max(blocks - 1, 1),)),
            ],
            compiler_params=pltpu.CompilerParams(collective_id=0, has_side_effects=True),
            name="slant_stack",
        )(traces, slopes.reshape(n_rx, own_slows), offsets[None], live[None])
        stack, coherence, peak = pl.pallas_call(
            emit,
            out_shape=shapes,
            in_specs=[vmem] * 3,
            out_specs=(anywhere,) * 3,
            scratch_shapes=[dma((3,))],
            name="emit",
        )(*results)
        return stack, coherence, peak[0]

    return jax.shard_map(
        on_device,
        mesh=mesh,
        in_specs=(P(("shots", "rx"), ("ta", "af")), P(), P("shots"), P("shots")),
        out_specs=(
            P(("shots", "rx"), ("ta", "af")),
            P(("shots", "rx"), ("ta", "af")),
            P(("shots", "rx")),
        ),
        check_vma=False,
    )
```

```python
import functools

import jax
import jax.numpy as jnp
from jax import lax
from jax.experimental import pallas as pl
from jax.experimental.pallas import tpu as pltpu
from jax.sharding import PartitionSpec as P

SPAN = 64
WIN = 16
STEP = 8
EDGE = SPAN + WIN
FAR = 3
MESH = pl.DeviceIdType.MESH
F32 = jnp.float32
BF16 = jnp.bfloat16


def window_sum(rows, width):
    reach = 1
    while reach < width:
        rows = rows[:-reach] + rows[reach:]
        reach *= 2
    return rows


def kernel(
    n_rx, n_ta, n_af, subs, pair,
    traces_hbm, slopes_hbm, offsets_hbm, live_hbm,
    stack_ref, coherence_ref, peak_ref,
    slopes_ref, offsets_ref, live_ref,
    held, delays, coming, long, left, total, edge_in, top, top_in,
    in_sem, small_sem, gather_recv, right_send, left_send, far_send, far_ready,
    edge_send, edge_recv, top_send, top_recv,
):
    blocks = n_ta * n_af
    sub_rows, block_len = held.shape[2:]
    own_slows = delays.shape[1]
    tall = block_len + STEP
    rx = lax.axis_index("rx")
    block = lax.axis_index("ta") * n_af + lax.axis_index("af")
    has_previous = block > 0
    has_next = block < blocks - 1
    has_left = rx > 0
    has_right = rx < n_rx - 1

    def at_block(number):
        return {"ta": lax.div(number, n_af), "af": lax.rem(number, n_af)}

    previous = at_block(jnp.maximum(block - 1, 0))
    block_peers = [at_block(lax.rem(block + step, blocks)) for step in range(1, blocks)]

    barrier = pltpu.get_barrier_semaphore()

    @pl.when(has_left)
    def _():
        pl.semaphore_signal(barrier, inc=1, device_id={"rx": rx - 1}, device_id_type=MESH)

    @pl.when(has_right)
    def _():
        pl.semaphore_signal(barrier, inc=1, device_id={"rx": rx + 1}, device_id_type=MESH)

    for peer in block_peers:
        pl.semaphore_signal(barrier, inc=1, device_id=peer, device_id_type=MESH)

    for reach in range(FAR, n_rx):
        @pl.when(rx + reach < n_rx)
        def _():
            pl.semaphore_signal(
                barrier, inc=1, device_id={"rx": jnp.minimum(rx + reach, n_rx - 1)},
                device_id_type=MESH)

    small = [
        pltpu.make_async_copy(source, target, small_sem.at[index])
        for index, (source, target) in enumerate(
            [(slopes_hbm, slopes_ref), (offsets_hbm, offsets_ref), (live_hbm, live_ref)])
    ]
    own = [
        pltpu.make_async_copy(
            traces_hbm.at[pl.ds(sub * sub_rows, sub_rows)], held.at[rx, sub], in_sem.at[sub])
        for sub in range(subs)
    ]
    for copy in small + own:
        copy.start()

    def to_right(source, sub):
        return pltpu.make_async_remote_copy(
            src_ref=held.at[source, sub], dst_ref=held.at[source, sub],
            send_sem=right_send.at[source, sub], recv_sem=gather_recv.at[source, sub],
            device_id={"rx": jnp.minimum(rx + 1, n_rx - 1)}, device_id_type=MESH,
        )

    def to_left(source, sub):
        return pltpu.make_async_remote_copy(
            src_ref=held.at[source, sub], dst_ref=held.at[source, sub],
            send_sem=left_send.at[source, sub], recv_sem=gather_recv.at[source, sub],
            device_id={"rx": jnp.maximum(rx - 1, 0)}, device_id_type=MESH,
        )

    def to_far(target, sub):
        return pltpu.make_async_remote_copy(
            src_ref=held.at[rx, sub], dst_ref=held.at[rx, sub],
            send_sem=far_send.at[target, sub], recv_sem=gather_recv.at[rx, sub],
            device_id={"rx": target}, device_id_type=MESH,
        )

    total[...] = jnp.zeros_like(total)
    long[0:STEP] = jnp.zeros((STEP, sub_rows), F32)
    long[block_len + STEP:] = jnp.zeros((STEP, sub_rows), F32)

    @pl.when(jnp.logical_not(has_next))
    def _():
        edge_in[...] = jnp.zeros_like(edge_in)

    for copy in small:
        copy.wait()

    near = jnp.where(has_left, 1, 0) + jnp.where(has_right, 1, 0)
    pl.semaphore_wait(barrier, near + blocks - 1 + jnp.maximum(rx - FAR + 1, 0))
    for sub in range(subs):
        own[sub].wait()

        @pl.when(has_right)
        def _():
            to_right(rx, sub).start()

        @pl.when(has_left)
        def _():
            to_left(rx, sub).start()

        for reach in range(FAR, n_rx):
            @pl.when(rx >= reach)
            def _():
                target = jnp.maximum(rx - reach, 0)
                to_far(target, sub).start()
                if sub == 0:
                    pl.semaphore_signal(
                        far_ready, inc=1, device_id={"rx": target}, device_id_type=MESH)

    slopes = slopes_ref[pl.ds(rx, 1), :].astype(F32)

    def delays_of(source, sub):
        lanes = pl.ds(pl.multiple_of((source * subs + sub) * sub_rows, sub_rows), sub_rows)
        offsets = offsets_ref[:, lanes].astype(F32)
        marked = jnp.where(live_ref[:, lanes] != 0, offsets, 65536.0)
        column = jnp.broadcast_to(marked, (128, sub_rows)).T
        column = jnp.concatenate([column] * (-(-own_slows // 128)), axis=1)[:, :own_slows]
        delay = jnp.floor(column * slopes * (1.0 / 65536.0))
        return jnp.where(column < 65536.0, delay, 127.0).astype(BF16)

    both = jnp.minimum(rx, n_rx - 1 - rx)

    def item_at(number):
        ahead = number - subs
        late = ahead - 2 * subs * both
        paired = late < 0
        spot = jnp.maximum(ahead, 0)
        tail = jnp.maximum(late, 0)
        place = lax.div(tail, subs)
        away = jnp.where(
            both == 0, jnp.where(place == 0, 0, n_rx - 1 - place), both + place)
        distance = jnp.where(paired, lax.div(spot, 2 * subs), away) + 1
        sub = jnp.where(paired, lax.div(lax.rem(spot, 2 * subs), 2), lax.rem(tail, subs))
        leftward = jnp.where(paired, 1 - lax.rem(spot, 2), jnp.where(rx > n_rx - 1 - rx, 1, 0))
        distance = jnp.where(leftward == 1, -distance, distance)
        mine = number < subs
        return jnp.where(mine, rx, rx + distance), jnp.where(mine, number, sub)

    def exchange(sub):
        before = jnp.maximum(rx - 1, 0)
        after = jnp.minimum(rx + 1, n_rx - 1)

        @pl.when(has_left)
        def _():
            to_right(before, sub).wait_recv()

            @pl.when(has_right)
            def _():
                to_right(before, sub).start()

        @pl.when(has_right)
        def _():
            to_left(after, sub).wait_recv()

            @pl.when(has_left)
            def _():
                to_left(after, sub).start()

    far_count = jnp.maximum(n_rx - FAR - rx, 0)

    def add_item(number, carry):
        source, sub = item_at(number)

        pace = jnp.where(both > 0, 2, 1)
        turn = lax.div(number - subs, pace)

        @pl.when(jnp.logical_and(
            number >= subs,
            jnp.logical_and(turn < subs, lax.rem(number - subs, pace) == 0)))
        def _():
            exchange(turn)

        @pl.when(jnp.abs(source - rx) > 1)
        def _():
            to_right(source, sub).wait_recv()

        @pl.when(jnp.logical_and(number == 1, far_count > 0))
        def _():
            pl.semaphore_wait(far_ready, far_count)
            for reach in range(FAR, n_rx):
                @pl.when(rx + reach < n_rx)
                def _():
                    for far_sub in range(subs):
                        to_far(jnp.minimum(rx + reach, n_rx - 1), far_sub).start()

        delays[...] = coming[...]
        long[STEP:STEP + block_len] = held[source, sub].astype(F32).T
        delay = delays[...]
        for lag in range(STEP):
            samples = long[lag:lag + tall]
            left[:, lag * sub_rows:(lag + 1) * sub_rows] = jnp.concatenate(
                [samples, samples * samples], axis=0).astype(BF16)
        for first in range(0, SPAN // STEP, pair):
            right = [
                jnp.concatenate([
                    jnp.where(delay == jnp.asarray(STEP * (first + turn) + lag, BF16),
                              jnp.asarray(1, BF16), jnp.asarray(0, BF16))
                    for turn in range(pair)], axis=1)
                for lag in range(STEP)
            ]
            product = jnp.dot(left[...], jnp.concatenate(right, axis=0),
                              preferred_element_type=F32)
            for turn in range(pair):
                top_row = SPAN - STEP * (first + turn + 1)
                lanes = slice(turn * own_slows, (turn + 1) * own_slows)
                total[0, top_row:top_row + tall] += product[:tall, lanes]
                total[1, top_row:top_row + tall] += product[tall:, lanes]
        coming[...] = delays_of(*item_at(jnp.minimum(number + 1, n_rx * subs - 1)))
        return carry

    coming[...] = delays_of(rx, 0)

    lax.fori_loop(0, n_rx * subs, add_item, 0)

    pass_edge = pltpu.make_async_remote_copy(
        src_ref=total.at[:, pl.ds(0, EDGE)], dst_ref=edge_in,
        send_sem=edge_send, recv_sem=edge_recv,
        device_id=previous, device_id_type=MESH,
    )

    @pl.when(has_previous)
    def _():
        pass_edge.start()

    @pl.when(has_next)
    def _():
        pass_edge.wait_recv()

    near_rows = block_len - SPAN

    def whole(kind):
        return jnp.concatenate([
            total[kind, SPAN:SPAN + near_rows],
            total[kind, SPAN + near_rows:] + edge_in[kind, 0:SPAN],
            edge_in[kind, SPAN:],
        ], axis=0)

    stack, energy = whole(0), whole(1)
    power_sum = window_sum(stack * stack, WIN)[:block_len]
    energy_sum = window_sum(energy, WIN)[:block_len]
    coherence = power_sum / jnp.maximum(energy_sum, 1.0)
    peak = jnp.max(coherence, axis=0, keepdims=True)
    top[...] = peak
    tops = []
    for step, peer in enumerate(block_peers):
        tops.append(pltpu.make_async_remote_copy(
            src_ref=top, dst_ref=top_in.at[step],
            send_sem=top_send.at[step], recv_sem=top_recv.at[step],
            device_id=peer, device_id_type=MESH,
        ))
        tops[-1].start()
    stack_ref[...] = stack[:block_len].T
    coherence_ref[...] = coherence.T

    for sub in range(subs):
        @pl.when(has_right)
        def _():
            to_right(rx, sub).wait_send()

        @pl.when(has_left)
        def _():
            to_left(rx, sub).wait_send()

        @pl.when(jnp.logical_and(has_left, has_right))
        def _():
            to_right(jnp.maximum(rx - 1, 0), sub).wait_send()
            to_left(jnp.minimum(rx + 1, n_rx - 1), sub).wait_send()

        for reach in range(FAR, n_rx):
            @pl.when(rx >= reach)
            def _():
                to_far(jnp.maximum(rx - reach, 0), sub).wait_send()

            @pl.when(rx + reach < n_rx)
            def _():
                to_far(jnp.minimum(rx + reach, n_rx - 1), sub).wait_send()

    @pl.when(has_previous)
    def _():
        pass_edge.wait_send()

    for step, copy in enumerate(tops):
        copy.wait_recv()
        peak = jnp.maximum(peak, top_in[step])
    peak_ref[...] = peak
    for copy in tops:
        copy.wait_send()


def emit(stack_ref, coherence_ref, peak_ref, stack_hbm, coherence_hbm, peak_hbm, sem):
    copies = [
        pltpu.make_async_copy(source, target, sem.at[index])
        for index, (source, target) in enumerate(
            [(stack_ref, stack_hbm), (coherence_ref, coherence_hbm), (peak_ref, peak_hbm)])
    ]
    for copy in copies:
        copy.start()
    for copy in copies:
        copy.wait()


def solution(mesh):
    n_rx, n_ta, n_af = (mesh.shape[name] for name in ("rx", "ta", "af"))

    def on_device(traces, slopes, offsets, live):
        local_rows, block_len = traces.shape
        subs = 2 if local_rows % 512 == 0 else 1
        sub_rows = local_rows // subs
        own_slows = slopes.shape[0] // n_rx
        pair = min(max(256 // own_slows, 1), SPAN // STEP)
        blocks = n_ta * n_af
        tall = block_len + STEP
        dma = pltpu.SemaphoreType.DMA
        vmem = pl.BlockSpec(memory_space=pltpu.VMEM)
        anywhere = pl.BlockSpec(memory_space=pl.ANY)
        shapes = (
            jax.ShapeDtypeStruct((own_slows, block_len), F32),
            jax.ShapeDtypeStruct((own_slows, block_len), F32),
            jax.ShapeDtypeStruct((1, own_slows), F32),
        )
        results = pl.pallas_call(
            functools.partial(kernel, n_rx, n_ta, n_af, subs, pair),
            out_shape=shapes,
            in_specs=[pl.BlockSpec(memory_space=pltpu.HBM)] * 4,
            out_specs=(vmem,) * 3,
            scratch_shapes=[
                pltpu.VMEM((n_rx, own_slows), jnp.int32),
                pltpu.VMEM((1, n_rx * local_rows), jnp.int32),
                pltpu.VMEM((1, n_rx * local_rows), jnp.int32),
                pltpu.VMEM((n_rx, subs, sub_rows, block_len), BF16),
                pltpu.VMEM((sub_rows, own_slows), BF16),
                pltpu.VMEM((sub_rows, own_slows), BF16),
                pltpu.VMEM((block_len + 2 * STEP, sub_rows), F32),
                pltpu.VMEM((2 * tall, STEP * sub_rows), BF16),
                pltpu.VMEM((2, block_len + SPAN, own_slows), F32),
                pltpu.VMEM((2, EDGE, own_slows), F32),
                pltpu.VMEM((1, own_slows), F32),
                pltpu.VMEM((max(blocks - 1, 1), 1, own_slows), F32),
                dma((subs,)), dma((3,)), dma((n_rx, subs)), dma((n_rx, subs)), dma((n_rx, subs)),
                dma((n_rx, subs)), pltpu.SemaphoreType.REGULAR,
                dma, dma,
                dma((max(blocks - 1, 1),)), dma((max(blocks - 1, 1),)),
            ],
            compiler_params=pltpu.CompilerParams(collective_id=0, has_side_effects=True, vmem_limit_bytes=16777216),
            name="slant_stack",
        )(*[pltpu.with_memory_space_constraint(a, pltpu.HBM) for a in (traces, slopes.reshape(n_rx, own_slows), offsets[None], live[None])])
        stack, coherence, peak = pl.pallas_call(
            emit,
            out_shape=shapes,
            in_specs=[vmem] * 3,
            out_specs=(anywhere,) * 3,
            scratch_shapes=[dma((3,))],
            compiler_params=pltpu.CompilerParams(vmem_limit_bytes=4194304),
            name="emit",
        )(*results)
        return stack, coherence, peak[0]

    return jax.shard_map(
        on_device,
        mesh=mesh,
        in_specs=(P(("shots", "rx"), ("ta", "af")), P(), P("shots"), P("shots")),
        out_specs=(
            P(("shots", "rx"), ("ta", "af")),
            P(("shots", "rx"), ("ta", "af")),
            P(("shots", "rx")),
        ),
        check_vma=False,
    )
```

```python
import functools

import jax
import jax.numpy as jnp
from jax import lax
from jax.experimental import pallas as pl
from jax.experimental.pallas import tpu as pltpu
from jax.sharding import PartitionSpec as P

SPAN = 64
WIN = 16
STEP = 8
EDGE = SPAN + WIN
FAR = 3
PUT_OFF = 1
MESH = pl.DeviceIdType.MESH
F32 = jnp.float32
BF16 = jnp.bfloat16


def window_sum(rows, width):
    reach = 1
    while reach < width:
        rows = rows[:-reach] + rows[reach:]
        reach *= 2
    return rows


def kernel(
    n_rx, n_ta, n_af, subs, pair, put_off,
    traces_hbm, slopes_hbm, offsets_hbm, live_hbm,
    stack_ref, coherence_ref, peak_ref,
    slopes_ref, offsets_ref, live_ref,
    held, coming, full, early, late, total, edge_in, top, top_in,
    in_sem, small_sem, gather_recv, right_send, left_send, far_send, far_ready,
    edge_send, edge_recv, top_send, top_recv,
):
    blocks = n_ta * n_af
    sub_rows, block_len = held.shape[2:]
    own_slows = coming.shape[1]
    tall = block_len + STEP
    rx = lax.axis_index("rx")
    block = lax.axis_index("ta") * n_af + lax.axis_index("af")
    has_previous = block > 0
    has_next = block < blocks - 1
    has_left = rx > 0
    has_right = rx < n_rx - 1

    def at_block(number):
        return {"ta": lax.div(number, n_af), "af": lax.rem(number, n_af)}

    previous = at_block(jnp.maximum(block - 1, 0))
    block_peers = [at_block(lax.rem(block + step, blocks)) for step in range(1, blocks)]

    barrier = pltpu.get_barrier_semaphore()

    @pl.when(has_left)
    def _():
        pl.semaphore_signal(barrier, inc=1, device_id={"rx": rx - 1}, device_id_type=MESH)

    @pl.when(has_right)
    def _():
        pl.semaphore_signal(barrier, inc=1, device_id={"rx": rx + 1}, device_id_type=MESH)

    for peer in block_peers:
        pl.semaphore_signal(barrier, inc=1, device_id=peer, device_id_type=MESH)

    for reach in range(FAR, n_rx):
        @pl.when(rx + reach < n_rx)
        def _():
            pl.semaphore_signal(
                barrier, inc=1, device_id={"rx": jnp.minimum(rx + reach, n_rx - 1)},
                device_id_type=MESH)

    small = [
        pltpu.make_async_copy(source, target, small_sem.at[index])
        for index, (source, target) in enumerate(
            [(slopes_hbm, slopes_ref), (offsets_hbm, offsets_ref), (live_hbm, live_ref)])
    ]
    own = [
        pltpu.make_async_copy(
            traces_hbm.at[pl.ds(sub * sub_rows, sub_rows)], held.at[rx, sub], in_sem.at[sub])
        for sub in range(subs)
    ]
    for copy in small + own:
        copy.start()

    def to_right(source, sub):
        return pltpu.make_async_remote_copy(
            src_ref=held.at[source, sub], dst_ref=held.at[source, sub],
            send_sem=right_send.at[source, sub], recv_sem=gather_recv.at[source, sub],
            device_id={"rx": jnp.minimum(rx + 1, n_rx - 1)}, device_id_type=MESH,
        )

    def to_left(source, sub):
        return pltpu.make_async_remote_copy(
            src_ref=held.at[source, sub], dst_ref=held.at[source, sub],
            send_sem=left_send.at[source, sub], recv_sem=gather_recv.at[source, sub],
            device_id={"rx": jnp.maximum(rx - 1, 0)}, device_id_type=MESH,
        )

    def to_far(target, sub):
        return pltpu.make_async_remote_copy(
            src_ref=held.at[rx, sub], dst_ref=held.at[rx, sub],
            send_sem=far_send.at[target, sub], recv_sem=gather_recv.at[rx, sub],
            device_id={"rx": target}, device_id_type=MESH,
        )

    total[...] = jnp.zeros_like(total)
    for _, long, _ in (full, early, late):
        long[0:STEP] = jnp.zeros((STEP, sub_rows), F32)
        long[block_len + STEP:] = jnp.zeros((STEP, sub_rows), F32)

    @pl.when(jnp.logical_not(has_next))
    def _():
        edge_in[...] = jnp.zeros_like(edge_in)

    for copy in small:
        copy.wait()

    near = jnp.where(has_left, 1, 0) + jnp.where(has_right, 1, 0)
    pl.semaphore_wait(barrier, near + blocks - 1 + jnp.maximum(rx - FAR + 1, 0))
    for sub in range(subs):
        own[sub].wait()

        @pl.when(has_right)
        def _():
            to_right(rx, sub).start()

        @pl.when(has_left)
        def _():
            to_left(rx, sub).start()

        for reach in range(FAR, n_rx):
            @pl.when(rx >= reach)
            def _():
                target = jnp.maximum(rx - reach, 0)
                to_far(target, sub).start()
                if sub == 0:
                    pl.semaphore_signal(
                        far_ready, inc=1, device_id={"rx": target}, device_id_type=MESH)

    slopes = slopes_ref[pl.ds(rx, 1), :].astype(F32)

    def delays_of(source, sub):
        lanes = pl.ds(pl.multiple_of((source * subs + sub) * sub_rows, sub_rows), sub_rows)
        offsets = offsets_ref[:, lanes].astype(F32)
        marked = jnp.where(live_ref[:, lanes] != 0, offsets, 65536.0)
        column = jnp.broadcast_to(marked, (128, sub_rows)).T
        column = jnp.concatenate([column] * (-(-own_slows // 128)), axis=1)[:, :own_slows]
        delay = jnp.floor(column * slopes * (1.0 / 65536.0))
        return jnp.where(column < 65536.0, delay, 127.0).astype(BF16)

    both = jnp.minimum(rx, n_rx - 1 - rx)

    def item_at(number):
        ahead = number - subs
        late = ahead - 2 * subs * both
        paired = late < 0
        spot = jnp.maximum(ahead, 0)
        tail = jnp.maximum(late, 0)
        place = lax.div(tail, subs)
        away = jnp.where(
            both == 0, jnp.where(place == 0, 0, n_rx - 1 - place), both + place)
        distance = jnp.where(paired, lax.div(spot, 2 * subs), away) + 1
        sub = jnp.where(paired, lax.div(lax.rem(spot, 2 * subs), 2), lax.rem(tail, subs))
        leftward = jnp.where(paired, 1 - lax.rem(spot, 2), jnp.where(rx > n_rx - 1 - rx, 1, 0))
        distance = jnp.where(leftward == 1, -distance, distance)
        mine = number < subs
        return jnp.where(mine, rx, rx + distance), jnp.where(mine, number, sub)

    far_count = jnp.maximum(n_rx - FAR - rx, 0)

    def exchange(sub):
        @pl.when(jnp.logical_and(sub == 0, far_count > 0))
        def _():
            pl.semaphore_wait(far_ready, far_count)
            for reach in range(FAR, n_rx):
                @pl.when(rx + reach < n_rx)
                def _():
                    for far_sub in range(subs):
                        to_far(jnp.minimum(rx + reach, n_rx - 1), far_sub).start()

        before = jnp.maximum(rx - 1, 0)
        after = jnp.minimum(rx + 1, n_rx - 1)

        @pl.when(has_left)
        def _():
            to_right(before, sub).wait_recv()

            @pl.when(has_right)
            def _():
                to_right(before, sub).start()

        @pl.when(has_right)
        def _():
            to_left(after, sub).wait_recv()

            @pl.when(has_left)
            def _():
                to_left(after, sub).start()

    def await_item(number, source, sub):
        pace = jnp.where(both > 0, 2, 1)
        ahead = number - subs
        turn = jnp.where(both > 0, lax.div(ahead, 2), ahead)

        @pl.when(jnp.logical_and(
            number >= subs, jnp.logical_and(turn < subs, turn * pace == ahead)))
        def _():
            exchange(turn)

        @pl.when(jnp.abs(source - rx) > 1)
        def _():
            to_right(source, sub).wait_recv()

    last = n_rx * subs - 1

    def add_rows(number, place, rows, buffers, arriving):
        low, high = rows
        size = high - low
        delays, long, left = buffers
        source, sub = place
        if arriving:
            await_item(number, source, sub)
        delays[...] = coming[...]
        long[STEP:STEP + block_len] = held[source, sub].astype(F32).T
        for lag in range(STEP):
            samples = long[lag + low:lag + high]
            left[:, lag * sub_rows:(lag + 1) * sub_rows] = jnp.concatenate(
                [samples, samples * samples], axis=0).astype(BF16)
        delay = delays[...]
        for first in range(0, SPAN // STEP, pair):
            right = [
                jnp.concatenate([
                    jnp.where(delay == jnp.asarray(STEP * (first + turn) + lag, BF16),
                              jnp.asarray(1, BF16), jnp.asarray(0, BF16))
                    for turn in range(pair)], axis=1)
                for lag in range(STEP)
            ]
            product = jnp.dot(left[...], jnp.concatenate(right, axis=0),
                              preferred_element_type=F32)
            for turn in range(pair):
                shift = SPAN - STEP * (first + turn + 1)
                lanes = slice(turn * own_slows, (turn + 1) * own_slows)
                total[0, shift + low:shift + high] += product[:size, lanes]
                total[1, shift + low:shift + high] += product[size:, lanes]

    def add_full(number, place):
        add_rows(number, place, (0, tall), full, True)
        following = item_at(number + 1)
        coming[...] = delays_of(*following)
        return following

    def add_early(number, place):
        add_rows(number, place, (0, EDGE), early, True)
        following = item_at(jnp.where(number == last, last + 1 - put_off, number + 1))
        coming[...] = delays_of(*following)
        return following

    def add_late(number, place):
        add_rows(number, place, (EDGE, tall), late, False)
        following = item_at(jnp.minimum(number + 1, last))
        coming[...] = delays_of(*following)
        return following

    coming[...] = delays_of(rx, 0)
    place = lax.fori_loop(0, last + 1 - put_off, add_full, (rx, jnp.int32(0)))
    place = lax.fori_loop(last + 1 - put_off, last + 1, add_early, place)

    pass_edge = pltpu.make_async_remote_copy(
        src_ref=total.at[:, pl.ds(0, EDGE)], dst_ref=edge_in,
        send_sem=edge_send, recv_sem=edge_recv,
        device_id=previous, device_id_type=MESH,
    )

    @pl.when(has_previous)
    def _():
        pass_edge.start()

    lax.fori_loop(last + 1 - put_off, last + 1, add_late, place)

    @pl.when(has_next)
    def _():
        pass_edge.wait_recv()

    near_rows = block_len - SPAN

    def whole(kind):
        return jnp.concatenate([
            total[kind, SPAN:SPAN + near_rows],
            total[kind, SPAN + near_rows:] + edge_in[kind, 0:SPAN],
            edge_in[kind, SPAN:],
        ], axis=0)

    stack, energy = whole(0), whole(1)
    power_sum = window_sum(stack * stack, WIN)[:block_len]
    energy_sum = window_sum(energy, WIN)[:block_len]
    coherence = power_sum / jnp.maximum(energy_sum, 1.0)
    peak = jnp.max(coherence, axis=0, keepdims=True)
    top[...] = peak
    tops = []
    for step, peer in enumerate(block_peers):
        tops.append(pltpu.make_async_remote_copy(
            src_ref=top, dst_ref=top_in.at[step],
            send_sem=top_send.at[step], recv_sem=top_recv.at[step],
            device_id=peer, device_id_type=MESH,
        ))
        tops[-1].start()
    stack_ref[...] = stack[:block_len].T
    coherence_ref[...] = coherence.T

    for sub in range(subs):
        @pl.when(has_right)
        def _():
            to_right(rx, sub).wait_send()

        @pl.when(has_left)
        def _():
            to_left(rx, sub).wait_send()

        @pl.when(jnp.logical_and(has_left, has_right))
        def _():
            to_right(jnp.maximum(rx - 1, 0), sub).wait_send()
            to_left(jnp.minimum(rx + 1, n_rx - 1), sub).wait_send()

        for reach in range(FAR, n_rx):
            @pl.when(rx >= reach)
            def _():
                to_far(jnp.maximum(rx - reach, 0), sub).wait_send()

            @pl.when(rx + reach < n_rx)
            def _():
                to_far(jnp.minimum(rx + reach, n_rx - 1), sub).wait_send()

    @pl.when(has_previous)
    def _():
        pass_edge.wait_send()

    for step, copy in enumerate(tops):
        copy.wait_recv()
        peak = jnp.maximum(peak, top_in[step])
    peak_ref[...] = peak
    for copy in tops:
        copy.wait_send()


def emit(stack_ref, coherence_ref, peak_ref, stack_hbm, coherence_hbm, peak_hbm, sem):
    copies = [
        pltpu.make_async_copy(source, target, sem.at[index])
        for index, (source, target) in enumerate(
            [(stack_ref, stack_hbm), (coherence_ref, coherence_hbm), (peak_ref, peak_hbm)])
    ]
    for copy in copies:
        copy.start()
    for copy in copies:
        copy.wait()


def solution(mesh):
    n_rx, n_ta, n_af = (mesh.shape[name] for name in ("rx", "ta", "af"))

    def on_device(traces, slopes, offsets, live):
        local_rows, block_len = traces.shape
        subs = 2 if local_rows % 512 == 0 else 1
        sub_rows = local_rows // subs
        own_slows = slopes.shape[0] // n_rx
        pair = min(max(256 // own_slows, 1), SPAN // STEP)
        blocks = n_ta * n_af
        tall = block_len + STEP
        put_off = min(PUT_OFF, n_rx * subs - 1)

        def working(rows):
            return (
                pltpu.VMEM((sub_rows, own_slows), BF16),
                pltpu.VMEM((block_len + 2 * STEP, sub_rows), F32),
                pltpu.VMEM((2 * rows, STEP * sub_rows), BF16),
            )

        dma = pltpu.SemaphoreType.DMA
        vmem = pl.BlockSpec(memory_space=pltpu.VMEM)
        anywhere = pl.BlockSpec(memory_space=pl.ANY)
        shapes = (
            jax.ShapeDtypeStruct((own_slows, block_len), F32),
            jax.ShapeDtypeStruct((own_slows, block_len), F32),
            jax.ShapeDtypeStruct((1, own_slows), F32),
        )
        results = pl.pallas_call(
            functools.partial(kernel, n_rx, n_ta, n_af, subs, pair, put_off),
            out_shape=shapes,
            in_specs=[pl.BlockSpec(memory_space=pltpu.HBM)] * 4,
            out_specs=(vmem,) * 3,
            scratch_shapes=[
                pltpu.VMEM((n_rx, own_slows), jnp.int32),
                pltpu.VMEM((1, n_rx * local_rows), jnp.int32),
                pltpu.VMEM((1, n_rx * local_rows), jnp.int32),
                pltpu.VMEM((n_rx, subs, sub_rows, block_len), BF16),
                pltpu.VMEM((sub_rows, own_slows), BF16),
                working(tall), working(EDGE), working(tall - EDGE),
                pltpu.VMEM((2, block_len + SPAN, own_slows), F32),
                pltpu.VMEM((2, EDGE, own_slows), F32),
                pltpu.VMEM((1, own_slows), F32),
                pltpu.VMEM((max(blocks - 1, 1), 1, own_slows), F32),
                dma((subs,)), dma((3,)), dma((n_rx, subs)), dma((n_rx, subs)), dma((n_rx, subs)),
                dma((n_rx, subs)), pltpu.SemaphoreType.REGULAR,
                dma, dma,
                dma((max(blocks - 1, 1),)), dma((max(blocks - 1, 1),)),
            ],
            compiler_params=pltpu.CompilerParams(collective_id=0, has_side_effects=True, vmem_limit_bytes=16777216),
            name="slant_stack",
        )(*[pltpu.with_memory_space_constraint(a, pltpu.HBM) for a in (traces, slopes.reshape(n_rx, own_slows), offsets[None], live[None])])
        stack, coherence, peak = pl.pallas_call(
            emit,
            out_shape=shapes,
            in_specs=[vmem] * 3,
            out_specs=(anywhere,) * 3,
            scratch_shapes=[dma((3,))],
            compiler_params=pltpu.CompilerParams(vmem_limit_bytes=4194304),
            name="emit",
        )(*results)
        return stack, coherence, peak[0]

    return jax.shard_map(
        on_device,
        mesh=mesh,
        in_specs=(P(("shots", "rx"), ("ta", "af")), P(), P("shots"), P("shots")),
        out_specs=(
            P(("shots", "rx"), ("ta", "af")),
            P(("shots", "rx"), ("ta", "af")),
            P(("shots", "rx")),
        ),
        check_vma=False,
    )
```

```python
import functools

import jax
import jax.numpy as jnp
from jax import lax
from jax.experimental import pallas as pl
from jax.experimental.pallas import tpu as pltpu
from jax.sharding import PartitionSpec as P

SPAN = 64
WIN = 16
STEP = 8
EDGE = SPAN + WIN
FAR = 3
PUT_OFF = 1
MESH = pl.DeviceIdType.MESH
F32 = jnp.float32
BF16 = jnp.bfloat16


def window_sum(rows, width):
    reach = 1
    while reach < width:
        rows = rows[:-reach] + rows[reach:]
        reach *= 2
    return rows


def kernel(
    n_rx, n_ta, n_af, subs, pair, put_off,
    traces_hbm, slopes_hbm, offsets_hbm, live_hbm,
    stack_ref, coherence_ref, peak_ref,
    slopes_ref, offsets_ref, live_ref,
    held, coming, full, early, late, total, edge_in, top, top_in,
    in_sem, small_sem, gather_recv, right_send, left_send, far_send, far_ready,
    edge_send, edge_recv, top_send, top_recv,
):
    blocks = n_ta * n_af
    sub_rows, block_len = held.shape[2:]
    own_slows = coming.shape[1]
    tall = block_len + STEP
    rx = lax.axis_index("rx")
    block = lax.axis_index("ta") * n_af + lax.axis_index("af")
    has_previous = block > 0
    has_next = block < blocks - 1
    has_left = rx > 0
    has_right = rx < n_rx - 1

    def at_block(number):
        return {"ta": lax.div(number, n_af), "af": lax.rem(number, n_af)}

    previous = at_block(jnp.maximum(block - 1, 0))
    block_peers = [at_block(lax.rem(block + step, blocks)) for step in range(1, blocks)]

    barrier = pltpu.get_barrier_semaphore()

    @pl.when(has_left)
    def _():
        pl.semaphore_signal(barrier, inc=1, device_id={"rx": rx - 1}, device_id_type=MESH)

    @pl.when(has_right)
    def _():
        pl.semaphore_signal(barrier, inc=1, device_id={"rx": rx + 1}, device_id_type=MESH)

    for peer in block_peers:
        pl.semaphore_signal(barrier, inc=1, device_id=peer, device_id_type=MESH)

    for reach in range(FAR, n_rx):
        @pl.when(rx + reach < n_rx)
        def _():
            pl.semaphore_signal(
                barrier, inc=1, device_id={"rx": jnp.minimum(rx + reach, n_rx - 1)},
                device_id_type=MESH)

    small = [
        pltpu.make_async_copy(source, target, small_sem.at[index])
        for index, (source, target) in enumerate(
            [(slopes_hbm, slopes_ref), (offsets_hbm, offsets_ref), (live_hbm, live_ref)])
    ]
    own = [
        pltpu.make_async_copy(
            traces_hbm.at[pl.ds(sub * sub_rows, sub_rows)], held.at[rx, sub], in_sem.at[sub])
        for sub in range(subs)
    ]
    for copy in small + own:
        copy.start()

    def to_right(source, sub):
        return pltpu.make_async_remote_copy(
            src_ref=held.at[source, sub], dst_ref=held.at[source, sub],
            send_sem=right_send.at[source, sub], recv_sem=gather_recv.at[source, sub],
            device_id={"rx": jnp.minimum(rx + 1, n_rx - 1)}, device_id_type=MESH,
        )

    def to_left(source, sub):
        return pltpu.make_async_remote_copy(
            src_ref=held.at[source, sub], dst_ref=held.at[source, sub],
            send_sem=left_send.at[source, sub], recv_sem=gather_recv.at[source, sub],
            device_id={"rx": jnp.maximum(rx - 1, 0)}, device_id_type=MESH,
        )

    def to_far(target, sub):
        return pltpu.make_async_remote_copy(
            src_ref=held.at[rx, sub], dst_ref=held.at[rx, sub],
            send_sem=far_send.at[target, sub], recv_sem=gather_recv.at[rx, sub],
            device_id={"rx": target}, device_id_type=MESH,
        )

    total[...] = jnp.zeros_like(total)
    for _, long, _ in (full, early, late):
        long[0:STEP] = jnp.zeros((STEP, sub_rows), F32)
        long[block_len + STEP:] = jnp.zeros((STEP, sub_rows), F32)

    @pl.when(jnp.logical_not(has_next))
    def _():
        edge_in[...] = jnp.zeros_like(edge_in)

    for copy in small:
        copy.wait()

    near = jnp.where(has_left, 1, 0) + jnp.where(has_right, 1, 0)
    pl.semaphore_wait(barrier, near + blocks - 1 + jnp.maximum(rx - FAR + 1, 0))
    for sub in range(subs):
        own[sub].wait()

        @pl.when(has_right)
        def _():
            to_right(rx, sub).start()

        if sub == 0:
            @pl.when(has_left)
            def _():
                to_left(rx, 0).start()

        for reach in range(FAR, n_rx):
            @pl.when(rx >= reach)
            def _():
                target = jnp.maximum(rx - reach, 0)
                to_far(target, sub).start()
                if sub == 0:
                    pl.semaphore_signal(
                        far_ready, inc=1, device_id={"rx": target}, device_id_type=MESH)

    for sub in range(1, subs):
        @pl.when(has_left)
        def _():
            to_left(rx, sub).start()

    slopes = slopes_ref[pl.ds(rx, 1), :].astype(F32)

    def delays_of(source, sub):
        lanes = pl.ds(pl.multiple_of((source * subs + sub) * sub_rows, sub_rows), sub_rows)
        offsets = offsets_ref[:, lanes].astype(F32)
        marked = jnp.where(live_ref[:, lanes] != 0, offsets, 65536.0)
        column = jnp.broadcast_to(marked, (128, sub_rows)).T
        column = jnp.concatenate([column] * (-(-own_slows // 128)), axis=1)[:, :own_slows]
        delay = jnp.floor(column * slopes * (1.0 / 65536.0))
        return jnp.where(column < 65536.0, delay, 127.0).astype(BF16)

    both = jnp.minimum(rx, n_rx - 1 - rx)

    def item_at(number):
        ahead = number - subs
        late = ahead - 2 * subs * both
        paired = late < 0
        spot = jnp.maximum(ahead, 0)
        tail = jnp.maximum(late, 0)
        place = lax.div(tail, subs)
        away = jnp.where(
            both == 0, jnp.where(place == 0, 0, n_rx - 1 - place), both + place)
        distance = jnp.where(paired, lax.div(spot, 2 * subs), away) + 1
        sub = jnp.where(paired, lax.div(lax.rem(spot, 2 * subs), 2), lax.rem(tail, subs))
        leftward = jnp.where(paired, 1 - lax.rem(spot, 2), jnp.where(rx > n_rx - 1 - rx, 1, 0))
        distance = jnp.where(leftward == 1, -distance, distance)
        mine = number < subs
        return jnp.where(mine, rx, rx + distance), jnp.where(mine, number, sub)

    far_count = jnp.maximum(n_rx - FAR - rx, 0)

    def exchange(sub, whole):
        @pl.when(jnp.logical_and(sub == 0, far_count > 0))
        def _():
            pl.semaphore_wait(far_ready, far_count)
            for reach in range(FAR, n_rx):
                @pl.when(rx + reach < n_rx)
                def _():
                    for far_sub in range(subs):
                        to_far(jnp.minimum(rx + reach, n_rx - 1), far_sub).start()

        before = jnp.maximum(rx - 1, 0)
        after = jnp.minimum(rx + 1, n_rx - 1)

        @pl.when(has_left)
        def _():
            to_right(before, sub).wait_recv()

            @pl.when(has_right)
            def _():
                to_right(before, sub).start()

        @pl.when(jnp.logical_and(has_right, jnp.logical_or(whole, sub > 0)))
        def _():
            to_left(after, sub).wait_recv()

            @pl.when(has_left)
            def _():
                to_left(after, sub).start()

    def await_item(number, source, sub):
        pace = jnp.where(both > 0, 2, 1)
        ahead = number - subs
        turn = jnp.where(both > 0, lax.div(ahead, 2), ahead)

        @pl.when(jnp.logical_and(
            number >= subs, jnp.logical_and(turn < subs, turn * pace == ahead)))
        def _():
            exchange(turn, both == 0)

        @pl.when(jnp.logical_and(both > 0, ahead == 1))
        def _():
            after = jnp.minimum(rx + 1, n_rx - 1)
            to_left(after, 0).wait_recv()
            to_left(after, 0).start()

        @pl.when(jnp.abs(source - rx) > 1)
        def _():
            to_right(source, sub).wait_recv()

    last = n_rx * subs - 1

    def add_rows(number, place, rows, buffers, arriving):
        low, high = rows
        size = high - low
        delays, long, left = buffers
        source, sub = place
        if arriving:
            await_item(number, source, sub)
        delays[...] = coming[...]
        long[STEP:STEP + block_len] = held[source, sub].astype(F32).T
        for lag in range(STEP):
            samples = long[lag + low:lag + high]
            left[:, lag * sub_rows:(lag + 1) * sub_rows] = jnp.concatenate(
                [samples, samples * samples], axis=0).astype(BF16)
        delay = delays[...]
        for first in range(0, SPAN // STEP, pair):
            right = [
                jnp.concatenate([
                    jnp.where(delay == jnp.asarray(STEP * (first + turn) + lag, BF16),
                              jnp.asarray(1, BF16), jnp.asarray(0, BF16))
                    for turn in range(pair)], axis=1)
                for lag in range(STEP)
            ]
            product = jnp.dot(left[...], jnp.concatenate(right, axis=0),
                              preferred_element_type=F32)
            for turn in range(pair):
                shift = SPAN - STEP * (first + turn + 1)
                lanes = slice(turn * own_slows, (turn + 1) * own_slows)
                total[0, shift + low:shift + high] += product[:size, lanes]
                total[1, shift + low:shift + high] += product[size:, lanes]

    def add_full(number, place):
        add_rows(number, place, (0, tall), full, True)
        following = item_at(number + 1)
        coming[...] = delays_of(*following)
        return following

    def add_early(number, place):
        add_rows(number, place, (0, EDGE), early, True)
        following = item_at(jnp.where(number == last, last + 1 - put_off, number + 1))
        coming[...] = delays_of(*following)
        return following

    def add_late(number, place):
        add_rows(number, place, (EDGE, tall), late, False)
        following = item_at(jnp.minimum(number + 1, last))
        coming[...] = delays_of(*following)
        return following

    coming[...] = delays_of(rx, 0)
    place = lax.fori_loop(0, last + 1 - put_off, add_full, (rx, jnp.int32(0)))
    place = lax.fori_loop(last + 1 - put_off, last + 1, add_early, place)

    pass_edge = pltpu.make_async_remote_copy(
        src_ref=total.at[:, pl.ds(0, EDGE)], dst_ref=edge_in,
        send_sem=edge_send, recv_sem=edge_recv,
        device_id=previous, device_id_type=MESH,
    )

    @pl.when(has_previous)
    def _():
        pass_edge.start()

    lax.fori_loop(last + 1 - put_off, last + 1, add_late, place)

    @pl.when(has_next)
    def _():
        pass_edge.wait_recv()

    near_rows = block_len - SPAN

    def whole(kind):
        return jnp.concatenate([
            total[kind, SPAN:SPAN + near_rows],
            total[kind, SPAN + near_rows:] + edge_in[kind, 0:SPAN],
            edge_in[kind, SPAN:],
        ], axis=0)

    stack, energy = whole(0), whole(1)
    power_sum = window_sum(stack * stack, WIN)[:block_len]
    energy_sum = window_sum(energy, WIN)[:block_len]
    coherence = power_sum / jnp.maximum(energy_sum, 1.0)
    peak = jnp.max(coherence, axis=0, keepdims=True)
    top[...] = peak
    tops = []
    for step, peer in enumerate(block_peers):
        tops.append(pltpu.make_async_remote_copy(
            src_ref=top, dst_ref=top_in.at[step],
            send_sem=top_send.at[step], recv_sem=top_recv.at[step],
            device_id=peer, device_id_type=MESH,
        ))
        tops[-1].start()
    stack_ref[...] = stack[:block_len].T
    coherence_ref[...] = coherence.T

    for sub in range(subs):
        @pl.when(has_right)
        def _():
            to_right(rx, sub).wait_send()

        @pl.when(has_left)
        def _():
            to_left(rx, sub).wait_send()

        @pl.when(jnp.logical_and(has_left, has_right))
        def _():
            to_right(jnp.maximum(rx - 1, 0), sub).wait_send()
            to_left(jnp.minimum(rx + 1, n_rx - 1), sub).wait_send()

        for reach in range(FAR, n_rx):
            @pl.when(rx >= reach)
            def _():
                to_far(jnp.maximum(rx - reach, 0), sub).wait_send()

            @pl.when(rx + reach < n_rx)
            def _():
                to_far(jnp.minimum(rx + reach, n_rx - 1), sub).wait_send()

    @pl.when(has_previous)
    def _():
        pass_edge.wait_send()

    for step, copy in enumerate(tops):
        copy.wait_recv()
        peak = jnp.maximum(peak, top_in[step])
    peak_ref[...] = peak
    for copy in tops:
        copy.wait_send()


def emit(stack_ref, coherence_ref, peak_ref, stack_hbm, coherence_hbm, peak_hbm, sem):
    copies = [
        pltpu.make_async_copy(source, target, sem.at[index])
        for index, (source, target) in enumerate(
            [(stack_ref, stack_hbm), (coherence_ref, coherence_hbm), (peak_ref, peak_hbm)])
    ]
    for copy in copies:
        copy.start()
    for copy in copies:
        copy.wait()


def solution(mesh):
    n_rx, n_ta, n_af = (mesh.shape[name] for name in ("rx", "ta", "af"))

    def on_device(traces, slopes, offsets, live):
        local_rows, block_len = traces.shape
        subs = 2 if local_rows % 512 == 0 else 1
        sub_rows = local_rows // subs
        own_slows = slopes.shape[0] // n_rx
        pair = min(max(256 // own_slows, 1), SPAN // STEP)
        blocks = n_ta * n_af
        tall = block_len + STEP
        put_off = min(PUT_OFF, n_rx * subs - 1)

        def working(rows):
            return (
                pltpu.VMEM((sub_rows, own_slows), BF16),
                pltpu.VMEM((block_len + 2 * STEP, sub_rows), F32),
                pltpu.VMEM((2 * rows, STEP * sub_rows), BF16),
            )

        dma = pltpu.SemaphoreType.DMA
        vmem = pl.BlockSpec(memory_space=pltpu.VMEM)
        anywhere = pl.BlockSpec(memory_space=pl.ANY)
        shapes = (
            jax.ShapeDtypeStruct((own_slows, block_len), F32),
            jax.ShapeDtypeStruct((own_slows, block_len), F32),
            jax.ShapeDtypeStruct((1, own_slows), F32),
        )
        results = pl.pallas_call(
            functools.partial(kernel, n_rx, n_ta, n_af, subs, pair, put_off),
            out_shape=shapes,
            in_specs=[pl.BlockSpec(memory_space=pltpu.HBM)] * 4,
            out_specs=(vmem,) * 3,
            scratch_shapes=[
                pltpu.VMEM((n_rx, own_slows), jnp.int32),
                pltpu.VMEM((1, n_rx * local_rows), jnp.int32),
                pltpu.VMEM((1, n_rx * local_rows), jnp.int32),
                pltpu.VMEM((n_rx, subs, sub_rows, block_len), BF16),
                pltpu.VMEM((sub_rows, own_slows), BF16),
                working(tall), working(EDGE), working(tall - EDGE),
                pltpu.VMEM((2, block_len + SPAN, own_slows), F32),
                pltpu.VMEM((2, EDGE, own_slows), F32),
                pltpu.VMEM((1, own_slows), F32),
                pltpu.VMEM((max(blocks - 1, 1), 1, own_slows), F32),
                dma((subs,)), dma((3,)), dma((n_rx, subs)), dma((n_rx, subs)), dma((n_rx, subs)),
                dma((n_rx, subs)), pltpu.SemaphoreType.REGULAR,
                dma, dma,
                dma((max(blocks - 1, 1),)), dma((max(blocks - 1, 1),)),
            ],
            compiler_params=pltpu.CompilerParams(collective_id=0, has_side_effects=True, vmem_limit_bytes=16777216),
            name="slant_stack",
        )(*[pltpu.with_memory_space_constraint(a, pltpu.HBM) for a in (traces, slopes.reshape(n_rx, own_slows), offsets[None], live[None])])
        stack, coherence, peak = pl.pallas_call(
            emit,
            out_shape=shapes,
            in_specs=[vmem] * 3,
            out_specs=(anywhere,) * 3,
            scratch_shapes=[dma((3,))],
            compiler_params=pltpu.CompilerParams(vmem_limit_bytes=4194304),
            name="emit",
        )(*results)
        return stack, coherence, peak[0]

    return jax.shard_map(
        on_device,
        mesh=mesh,
        in_specs=(P(("shots", "rx"), ("ta", "af")), P(), P("shots"), P("shots")),
        out_specs=(
            P(("shots", "rx"), ("ta", "af")),
            P(("shots", "rx"), ("ta", "af")),
            P(("shots", "rx")),
        ),
        check_vma=False,
    )
```

```python
import functools

import jax
import jax.numpy as jnp
from jax import lax
from jax.experimental import pallas as pl
from jax.experimental.pallas import tpu as pltpu
from jax.sharding import PartitionSpec as P

SPAN = 64
WIN = 16
STEP = 8
EDGE = SPAN + WIN
FAR = 3
PUT_OFF = 1
MESH = pl.DeviceIdType.MESH
F32 = jnp.float32
BF16 = jnp.bfloat16


def window_sum(rows, width):
    reach = 1
    while reach < width:
        rows = rows[:-reach] + rows[reach:]
        reach *= 2
    return rows


def kernel(
    n_rx, n_ta, n_af, subs, pair, most_put_off,
    traces_hbm, slopes_hbm, offsets_hbm, live_hbm,
    stack_ref, coherence_ref, peak_ref,
    slopes_ref, offsets_ref, live_ref,
    held, coming, full, early, late, total, edge_in, top, top_in,
    in_sem, small_sem, gather_recv, right_send, left_send, far_send, far_ready,
    edge_send, edge_recv, top_send, top_recv,
):
    blocks = n_ta * n_af
    sub_rows, block_len = held.shape[2:]
    own_slows = coming.shape[1]
    tall = block_len + STEP
    rx = lax.axis_index("rx")
    block = lax.axis_index("ta") * n_af + lax.axis_index("af")
    has_previous = block > 0
    has_next = block < blocks - 1
    has_left = rx > 0
    has_right = rx < n_rx - 1

    def at_block(number):
        return {"ta": lax.div(number, n_af), "af": lax.rem(number, n_af)}

    previous = at_block(jnp.maximum(block - 1, 0))
    block_peers = [at_block(lax.rem(block + step, blocks)) for step in range(1, blocks)]

    barrier = pltpu.get_barrier_semaphore()

    @pl.when(has_left)
    def _():
        pl.semaphore_signal(barrier, inc=1, device_id={"rx": rx - 1}, device_id_type=MESH)

    @pl.when(has_right)
    def _():
        pl.semaphore_signal(barrier, inc=1, device_id={"rx": rx + 1}, device_id_type=MESH)

    for peer in block_peers:
        pl.semaphore_signal(barrier, inc=1, device_id=peer, device_id_type=MESH)

    for reach in range(FAR, n_rx):
        @pl.when(rx + reach < n_rx)
        def _():
            pl.semaphore_signal(
                barrier, inc=1, device_id={"rx": jnp.minimum(rx + reach, n_rx - 1)},
                device_id_type=MESH)

    small = [
        pltpu.make_async_copy(source, target, small_sem.at[index])
        for index, (source, target) in enumerate(
            [(slopes_hbm, slopes_ref), (offsets_hbm, offsets_ref), (live_hbm, live_ref)])
    ]
    own = [
        pltpu.make_async_copy(
            traces_hbm.at[pl.ds(sub * sub_rows, sub_rows)], held.at[rx, sub], in_sem.at[sub])
        for sub in range(subs)
    ]
    for copy in small + own:
        copy.start()

    def to_right(source, sub):
        return pltpu.make_async_remote_copy(
            src_ref=held.at[source, sub], dst_ref=held.at[source, sub],
            send_sem=right_send.at[source, sub], recv_sem=gather_recv.at[source, sub],
            device_id={"rx": jnp.minimum(rx + 1, n_rx - 1)}, device_id_type=MESH,
        )

    def to_left(source, sub):
        return pltpu.make_async_remote_copy(
            src_ref=held.at[source, sub], dst_ref=held.at[source, sub],
            send_sem=left_send.at[source, sub], recv_sem=gather_recv.at[source, sub],
            device_id={"rx": jnp.maximum(rx - 1, 0)}, device_id_type=MESH,
        )

    def to_far(target, sub):
        return pltpu.make_async_remote_copy(
            src_ref=held.at[rx, sub], dst_ref=held.at[rx, sub],
            send_sem=far_send.at[target, sub], recv_sem=gather_recv.at[rx, sub],
            device_id={"rx": target}, device_id_type=MESH,
        )

    total[...] = jnp.zeros_like(total)
    for _, long, _ in (full, early, late):
        long[0:STEP] = jnp.zeros((STEP, sub_rows), F32)
        long[block_len + STEP:] = jnp.zeros((STEP, sub_rows), F32)

    @pl.when(jnp.logical_not(has_next))
    def _():
        edge_in[...] = jnp.zeros_like(edge_in)

    for copy in small:
        copy.wait()

    near = jnp.where(has_left, 1, 0) + jnp.where(has_right, 1, 0)
    pl.semaphore_wait(barrier, near + blocks - 1 + jnp.maximum(rx - FAR + 1, 0))
    for sub in range(subs):
        own[sub].wait()

        @pl.when(has_right)
        def _():
            to_right(rx, sub).start()

        if sub == 0:
            @pl.when(has_left)
            def _():
                to_left(rx, 0).start()

        for reach in range(FAR, n_rx):
            @pl.when(rx >= reach)
            def _():
                target = jnp.maximum(rx - reach, 0)
                to_far(target, sub).start()
                if sub == 0:
                    pl.semaphore_signal(
                        far_ready, inc=1, device_id={"rx": target}, device_id_type=MESH)

    for sub in range(1, subs):
        @pl.when(has_left)
        def _():
            to_left(rx, sub).start()

    slopes = slopes_ref[pl.ds(rx, 1), :].astype(F32)

    def delays_of(source, sub):
        lanes = pl.ds(pl.multiple_of((source * subs + sub) * sub_rows, sub_rows), sub_rows)
        offsets = offsets_ref[:, lanes].astype(F32)
        marked = jnp.where(live_ref[:, lanes] != 0, offsets, 65536.0)
        column = jnp.broadcast_to(marked, (128, sub_rows)).T
        column = jnp.concatenate([column] * (-(-own_slows // 128)), axis=1)[:, :own_slows]
        delay = jnp.floor(column * slopes * (1.0 / 65536.0))
        return jnp.where(column < 65536.0, delay, 127.0).astype(BF16)

    both = jnp.minimum(rx, n_rx - 1 - rx)

    def item_at(number):
        ahead = number - subs
        late = ahead - 2 * subs * both
        paired = late < 0
        spot = jnp.maximum(ahead, 0)
        tail = jnp.maximum(late, 0)
        place = lax.div(tail, subs)
        away = jnp.where(
            both == 0, jnp.where(place == 0, 0, n_rx - 1 - place), both + place)
        distance = jnp.where(paired, lax.div(spot, 2 * subs), away) + 1
        sub = jnp.where(paired, lax.div(lax.rem(spot, 2 * subs), 2), lax.rem(tail, subs))
        leftward = jnp.where(paired, 1 - lax.rem(spot, 2), jnp.where(rx > n_rx - 1 - rx, 1, 0))
        distance = jnp.where(leftward == 1, -distance, distance)
        mine = number < subs
        return jnp.where(mine, rx, rx + distance), jnp.where(mine, number, sub)

    far_count = jnp.maximum(n_rx - FAR - rx, 0)

    def exchange(sub, whole):
        @pl.when(jnp.logical_and(sub == 0, far_count > 0))
        def _():
            pl.semaphore_wait(far_ready, far_count)
            for reach in range(FAR, n_rx):
                @pl.when(rx + reach < n_rx)
                def _():
                    for far_sub in range(subs):
                        to_far(jnp.minimum(rx + reach, n_rx - 1), far_sub).start()

        before = jnp.maximum(rx - 1, 0)
        after = jnp.minimum(rx + 1, n_rx - 1)

        @pl.when(has_left)
        def _():
            to_right(before, sub).wait_recv()

            @pl.when(has_right)
            def _():
                to_right(before, sub).start()

        @pl.when(jnp.logical_and(has_right, jnp.logical_or(whole, sub > 0)))
        def _():
            to_left(after, sub).wait_recv()

            @pl.when(has_left)
            def _():
                to_left(after, sub).start()

    def await_item(number, source, sub):
        pace = jnp.where(both > 0, 2, 1)
        ahead = number - subs
        turn = jnp.where(both > 0, lax.div(ahead, 2), ahead)

        @pl.when(jnp.logical_and(
            number >= subs, jnp.logical_and(turn < subs, turn * pace == ahead)))
        def _():
            exchange(turn, both == 0)

        @pl.when(jnp.logical_and(both > 0, ahead == 1))
        def _():
            after = jnp.minimum(rx + 1, n_rx - 1)
            to_left(after, 0).wait_recv()
            to_left(after, 0).start()

        @pl.when(jnp.abs(source - rx) > 1)
        def _():
            to_right(source, sub).wait_recv()

    last = n_rx * subs - 1
    crossing = jnp.logical_and(has_previous, lax.axis_index("af") == 0)
    put_off = jnp.where(crossing, most_put_off, 0)

    def add_rows(number, place, rows, buffers, arriving):
        low, high = rows
        size = high - low
        delays, long, left = buffers
        source, sub = place
        if arriving:
            await_item(number, source, sub)
        delays[...] = coming[...]
        long[STEP:STEP + block_len] = held[source, sub].astype(F32).T
        for lag in range(STEP):
            samples = long[lag + low:lag + high]
            left[:, lag * sub_rows:(lag + 1) * sub_rows] = jnp.concatenate(
                [samples, samples * samples], axis=0).astype(BF16)
        delay = delays[...]
        for first in range(0, SPAN // STEP, pair):
            right = [
                jnp.concatenate([
                    jnp.where(delay == jnp.asarray(STEP * (first + turn) + lag, BF16),
                              jnp.asarray(1, BF16), jnp.asarray(0, BF16))
                    for turn in range(pair)], axis=1)
                for lag in range(STEP)
            ]
            product = jnp.dot(left[...], jnp.concatenate(right, axis=0),
                              preferred_element_type=F32)
            for turn in range(pair):
                shift = SPAN - STEP * (first + turn + 1)
                lanes = slice(turn * own_slows, (turn + 1) * own_slows)
                total[0, shift + low:shift + high] += product[:size, lanes]
                total[1, shift + low:shift + high] += product[size:, lanes]

    def add_full(number, place):
        add_rows(number, place, (0, tall), full, True)
        following = item_at(jnp.minimum(number + 1, last))
        coming[...] = delays_of(*following)
        return following

    def add_early(number, place):
        add_rows(number, place, (0, EDGE), early, True)
        following = item_at(jnp.where(number == last, last + 1 - put_off, number + 1))
        coming[...] = delays_of(*following)
        return following

    def add_late(number, place):
        add_rows(number, place, (EDGE, tall), late, False)
        following = item_at(jnp.minimum(number + 1, last))
        coming[...] = delays_of(*following)
        return following

    coming[...] = delays_of(rx, 0)
    place = lax.fori_loop(0, last + 1 - put_off, add_full, (rx, jnp.int32(0)))
    place = lax.fori_loop(last + 1 - put_off, last + 1, add_early, place)

    def pass_edge(kind):
        return pltpu.make_async_remote_copy(
            src_ref=total.at[kind, pl.ds(0, EDGE)], dst_ref=edge_in.at[kind],
            send_sem=edge_send.at[kind], recv_sem=edge_recv.at[kind],
            device_id=previous, device_id_type=MESH,
        )

    @pl.when(has_previous)
    def _():
        for kind in range(2):
            pass_edge(kind).start()

    lax.fori_loop(last + 1 - put_off, last + 1, add_late, place)

    near_rows = block_len - SPAN
    sure = near_rows - WIN

    def near(kind):
        return total[kind, SPAN:block_len]

    def far(kind):
        @pl.when(has_next)
        def _():
            pass_edge(kind).wait_recv()

        return jnp.concatenate([
            total[kind, SPAN + sure:block_len],
            total[kind, block_len:] + edge_in[kind, 0:SPAN],
            edge_in[kind, SPAN:],
        ], axis=0)

    def windows(rows):
        return window_sum(rows, WIN)[:rows.shape[0] - WIN]

    near_stack = near(0)
    near_coherence = windows(near_stack * near_stack) / jnp.maximum(windows(near(1)), 1.0)
    far_stack = far(0)
    far_power = windows(far_stack * far_stack)
    far_coherence = far_power / jnp.maximum(windows(far(1)), 1.0)
    stack = jnp.concatenate([near_stack[:sure], far_stack], axis=0)
    coherence = jnp.concatenate([near_coherence, far_coherence], axis=0)
    peak = jnp.max(coherence, axis=0, keepdims=True)
    top[...] = peak
    tops = []
    for step, peer in enumerate(block_peers):
        tops.append(pltpu.make_async_remote_copy(
            src_ref=top, dst_ref=top_in.at[step],
            send_sem=top_send.at[step], recv_sem=top_recv.at[step],
            device_id=peer, device_id_type=MESH,
        ))
        tops[-1].start()
    stack_ref[...] = stack[:block_len].T
    coherence_ref[...] = coherence.T

    for sub in range(subs):
        @pl.when(has_right)
        def _():
            to_right(rx, sub).wait_send()

        @pl.when(has_left)
        def _():
            to_left(rx, sub).wait_send()

        @pl.when(jnp.logical_and(has_left, has_right))
        def _():
            to_right(jnp.maximum(rx - 1, 0), sub).wait_send()
            to_left(jnp.minimum(rx + 1, n_rx - 1), sub).wait_send()

        for reach in range(FAR, n_rx):
            @pl.when(rx >= reach)
            def _():
                to_far(jnp.maximum(rx - reach, 0), sub).wait_send()

            @pl.when(rx + reach < n_rx)
            def _():
                to_far(jnp.minimum(rx + reach, n_rx - 1), sub).wait_send()

    @pl.when(has_previous)
    def _():
        for kind in range(2):
            pass_edge(kind).wait_send()

    for step, copy in enumerate(tops):
        copy.wait_recv()
        peak = jnp.maximum(peak, top_in[step])
    peak_ref[...] = peak
    for copy in tops:
        copy.wait_send()


def emit(stack_ref, coherence_ref, peak_ref, stack_hbm, coherence_hbm, peak_hbm, sem):
    copies = [
        pltpu.make_async_copy(source, target, sem.at[index])
        for index, (source, target) in enumerate(
            [(stack_ref, stack_hbm), (coherence_ref, coherence_hbm), (peak_ref, peak_hbm)])
    ]
    for copy in copies:
        copy.start()
    for copy in copies:
        copy.wait()


def solution(mesh):
    n_rx, n_ta, n_af = (mesh.shape[name] for name in ("rx", "ta", "af"))

    def on_device(traces, slopes, offsets, live):
        local_rows, block_len = traces.shape
        subs = 2 if local_rows % 512 == 0 else 1
        sub_rows = local_rows // subs
        own_slows = slopes.shape[0] // n_rx
        pair = min(max(256 // own_slows, 1), SPAN // STEP)
        blocks = n_ta * n_af
        tall = block_len + STEP
        put_off = min(PUT_OFF, n_rx * subs - 1)

        def working(rows):
            return (
                pltpu.VMEM((sub_rows, own_slows), BF16),
                pltpu.VMEM((block_len + 2 * STEP, sub_rows), F32),
                pltpu.VMEM((2 * rows, STEP * sub_rows), BF16),
            )

        dma = pltpu.SemaphoreType.DMA
        vmem = pl.BlockSpec(memory_space=pltpu.VMEM)
        anywhere = pl.BlockSpec(memory_space=pl.ANY)
        shapes = (
            jax.ShapeDtypeStruct((own_slows, block_len), F32),
            jax.ShapeDtypeStruct((own_slows, block_len), F32),
            jax.ShapeDtypeStruct((1, own_slows), F32),
        )
        results = pl.pallas_call(
            functools.partial(kernel, n_rx, n_ta, n_af, subs, pair, put_off),
            out_shape=shapes,
            in_specs=[pl.BlockSpec(memory_space=pltpu.HBM)] * 4,
            out_specs=(vmem,) * 3,
            scratch_shapes=[
                pltpu.VMEM((n_rx, own_slows), jnp.int32),
                pltpu.VMEM((1, n_rx * local_rows), jnp.int32),
                pltpu.VMEM((1, n_rx * local_rows), jnp.int32),
                pltpu.VMEM((n_rx, subs, sub_rows, block_len), BF16),
                pltpu.VMEM((sub_rows, own_slows), BF16),
                working(tall), working(EDGE), working(tall - EDGE),
                pltpu.VMEM((2, block_len + SPAN, own_slows), F32),
                pltpu.VMEM((2, EDGE, own_slows), F32),
                pltpu.VMEM((1, own_slows), F32),
                pltpu.VMEM((max(blocks - 1, 1), 1, own_slows), F32),
                dma((subs,)), dma((3,)), dma((n_rx, subs)), dma((n_rx, subs)), dma((n_rx, subs)),
                dma((n_rx, subs)), pltpu.SemaphoreType.REGULAR,
                dma((2,)), dma((2,)),
                dma((max(blocks - 1, 1),)), dma((max(blocks - 1, 1),)),
            ],
            compiler_params=pltpu.CompilerParams(collective_id=0, has_side_effects=True, vmem_limit_bytes=16777216),
            name="slant_stack",
        )(*[pltpu.with_memory_space_constraint(a, pltpu.HBM) for a in (traces, slopes.reshape(n_rx, own_slows), offsets[None], live[None])])
        stack, coherence, peak = pl.pallas_call(
            emit,
            out_shape=shapes,
            in_specs=[vmem] * 3,
            out_specs=(anywhere,) * 3,
            scratch_shapes=[dma((3,))],
            compiler_params=pltpu.CompilerParams(vmem_limit_bytes=4194304),
            name="emit",
        )(*results)
        return stack, coherence, peak[0]

    return jax.shard_map(
        on_device,
        mesh=mesh,
        in_specs=(P(("shots", "rx"), ("ta", "af")), P(), P("shots"), P("shots")),
        out_specs=(
            P(("shots", "rx"), ("ta", "af")),
            P(("shots", "rx"), ("ta", "af")),
            P(("shots", "rx")),
        ),
        check_vma=False,
    )
```
